1024 devices in a mesh: row: 64 (over y, x), col: 16 (over z, core).
Axes of the slice: x: 8, y: 8, z: 8, core: 2. Of those that a mesh axis runs over, the one named last changes fastest.
Arguments:
- points: bfloat16 [16, 16384, 768], P('col', 'row'), may hold values from -6 to 6
- candidates: int32 [16, 2048, 4], P('col', 'row'), may hold values from 0 to 63, all different within a row; in each aligned block of 32 rows (0 to 31, 32 to 63, ..., all dimensions but the last counted through in order) at most 4 rows name the same one
- centroids: float32 [64, 256, 768], P('row'), may hold values from -2 to 2
- prices: float32 [64, 256], P('row'), may hold values from -1 to 1
Outputs:
- new_centroids: float32 [64, 256, 768], P('row')
- new_prices: float32 [64, 256], P('row')
The draws below stay inside these ranges and needn't reach their ends.
Inputs may be any that keep to these rules, and one draw needn't show every extreme that they name: `candidates`: each block names 4 different cells. Among the 32 blocks of one device no cell is named by more than 4 blocks, and in every draw some device has a cell named by exactly 4 of its blocks.
All inputs are finite; a program needn't handle non-finite values.
Results may differ from the reference program's by a relative error of at most 0.0065.
The reference program's roundings to bfloat16 on the way count: a program that leaves them out, or rounds other values in their place, can miss the bound.
Values may be sent and summed in bfloat16 or wider, within the bound.
No kernel may reach another device: no remote copies, remote signals or barrier semaphores. Data moves between devices by JAX's collectives and lax.ppermute only.
A program may use at most 64 MiB of HBM per device.

```python
import math
import jax
import jax.numpy as jnp
import numpy as np
from jax import lax

D = 768
CENT = 256
TOP = 4
BLK = 8
STEPS = 2
BLOCKS = 32
CAP = 4
CELLS = 64
N_ROW = 64
N_COL = 16


def draw_centroids(key, part):
    noise = 0.06 * jax.random.normal(jax.random.fold_in(key, 7011), (CELLS, CENT, D), jnp.float32)
    values = jnp.clip(noise, -0.36, 0.36)
    return values.astype(jnp.float32)


def draw_points(key, part):
    rows = N_ROW * BLOCKS * BLK
    values = jax.random.normal(jax.random.fold_in(key, 7025), (N_COL, rows, D), jnp.float32)
    return jnp.clip(values, -6.0, 6.0).astype(jnp.bfloat16)


def block_scale(own_key, shape, cuts, least, high):
    gain = 1.0
    for position, shards_of in cuts:
        heights = jax.random.uniform(jax.random.fold_in(jax.random.fold_in(own_key, 6), position), (shards_of,), jnp.float32, least / len(cuts), high / len(cuts))
        gain = gain * jnp.repeat(jnp.exp(heights), shape[position] // shards_of).reshape((-1,) + (1,) * (len(shape) - 1 - position))
    return gain


def assign_block(own_key, own, number, rows, amount, top, most, skew):
    order = jax.random.permutation(own_key, amount)
    crowded, ordinary = load_shares(amount, rows * top, most, skew, True), load_shares(amount, rows * top, most, skew, False)
    places = jnp.arange(amount)

    def named(tallies, turn):
        used = int((tallies > 0).sum())
        fixed = max(1, used // 4)
        shifted = fixed + (places - fixed + turn * (used - fixed)) % max(1, amount - fixed)
        return jnp.zeros((amount,), jnp.int32).at[order[jnp.where(places < fixed, places, shifted)]].set(jnp.asarray(tallies, jnp.int32))

    tallies = jnp.where(number % 4 == 0, named(crowded, number // 4), named(ordinary, number - number // 4 - 1))
    mixed = jax.random.permutation(jax.random.fold_in(own, 3), amount)
    source_of, sink = mixed[0:amount // 2 * 2:2], mixed[1:amount // 2 * 2:2]
    room = jnp.minimum(tallies[source_of] - 1, most - tallies[sink]) // 2
    room = jnp.where((source_of == order[0]) | (sink == order[0]) | (tallies[sink] == 0), 0, jnp.maximum(room, 0))
    shifted = jax.random.randint(jax.random.fold_in(own, 4), (amount // 2,), 0, 1 << 20) % (room + 1)
    tallies = tallies.at[source_of].add(-shifted).at[sink].add(shifted)
    members = jnp.searchsorted(jnp.cumsum(tallies), jnp.arange(rows * top), side="right").astype(jnp.int32)
    table = members.reshape(top, rows).T
    table = table[jax.random.permutation(jax.random.fold_in(own, 1), rows)]
    turn = jax.random.randint(jax.random.fold_in(own, 2), (rows, 1), 0, top)
    return jnp.take_along_axis(table, (jnp.arange(top)[None, :] + turn) % top, axis=1)


def load_shares(count, total, reach, slope, full):
    portions = [(1 << 20) // math.isqrt(rank ** slope) + 1 for rank in range(1, count + 1)]
    largest = reach if full else min(reach, max(-(-total // count), total * portions[0] // sum(portions)))
    least = 1 if total - largest >= count - 1 else 0
    holding, spare = [largest] + [least] * (count - 1), total - largest - least * (count - 1)
    while spare > 0:
        movable = [i for i in range(1, count) if holding[i] < largest] or [i for i in range(1, count) if holding[i] < reach]
        pool, remaining = sum([portions[i] for i in movable]), spare
        for i in movable:
            more = min(reach - holding[i], max(1, remaining * portions[i] // pool), spare)
            holding[i] = holding[i] + more
            spare = spare - more
    return np.array(holding)


def setup_inputs(seed: int = 0) -> dict:
    streams_of = jax.random.split(jax.random.key(seed), 5)
    points = draw_points(jax.random.fold_in(streams_of[4], 71), 0)
    candidates_keys = jax.random.split(jax.random.fold_in(streams_of[1], 1), N_COL * (N_ROW * BLOCKS) // BLOCKS)
    candidates_turns = jax.random.permutation(jax.random.fold_in(streams_of[1], 3), N_COL * (N_ROW * BLOCKS) // BLOCKS)
    candidates = jax.vmap(lambda own, number: assign_block(jax.random.fold_in(streams_of[1], 2), own, number, BLOCKS, N_ROW, TOP, CAP, 2))(candidates_keys, candidates_turns).reshape((N_COL, N_ROW * BLOCKS, TOP))
    centroids = draw_centroids(jax.random.fold_in(streams_of[4], 71), 0)
    prices = jnp.clip(jax.random.uniform(streams_of[3], (CELLS, CENT), jnp.float32, -1.0, 1.0) * block_scale(streams_of[3], (CELLS, CENT), ((0, 64),), -0.4, 0.0), -1.0, 1.0)
    return dict(points=points, candidates=candidates, centroids=centroids, prices=prices)


prior_mass = 1.0
price_rate = 0.5


def reference(points, candidates, centroids, prices):
    groups = N_ROW * BLOCKS
    listed = N_ROW * CAP
    cell_ids = jnp.arange(N_ROW, dtype=jnp.int32)
    columns = jnp.arange(N_COL, dtype=jnp.int32)
    named = jnp.any(candidates[:, :, :, None] == cell_ids[None, None, None, :], axis=2)
    named_cells = jnp.transpose(named, (2, 0, 1))
    order = jnp.arange(groups, dtype=jnp.int32)
    sort_keys = jnp.where(named_cells, order, order + groups)
    picked = jnp.argsort(sort_keys, axis=-1)[:, :, :listed].astype(jnp.int32)
    present = jnp.take_along_axis(named_cells, picked, axis=-1)
    blocks = points.reshape(N_COL, groups, BLK, D)
    point_ids = ((columns[None, :, None] * groups + picked)[..., None] * BLK
                 + jnp.arange(BLK, dtype=jnp.int32)).reshape(N_ROW, N_COL, listed * BLK)
    row_mask = jnp.repeat(present, BLK, axis=-1).astype(jnp.float32)
    total_points = N_COL * groups * BLK
    target = N_COL * BLOCKS * BLK / CENT
    means = centroids
    price = prices
    for sweep_index in range(STEPS):
        means_half = means.astype(jnp.bfloat16)
        offset = 0.5 * jnp.sum(means * means, axis=-1) + price

        def scores_of(which_cell, column, chosen):
            point_rows = blocks[column][chosen].reshape(listed * BLK, D)
            scores = jnp.dot(point_rows, means_half[which_cell].T, preferred_element_type=jnp.float32)
            return point_rows, scores - offset[which_cell][None, :]

        def stats_cell(args):
            which_cell, chosen_all = args

            def per_column(items):
                column, chosen = items
                unused, scores = scores_of(which_cell, column, chosen)
                highest = jnp.max(scores, axis=-1)
                return highest, jnp.sum(jnp.exp(scores - highest[:, None]), axis=-1)

            return lax.map(per_column, (columns, chosen_all))

        highest, masses = lax.map(stats_cell, (cell_ids, picked))
        flat_ids = point_ids.reshape(-1)
        flat_mask = row_mask.reshape(-1)
        masked_top = jnp.where(flat_mask > 0, highest.reshape(-1), jnp.float32(-1e30))
        largest = jnp.full((total_points,), -1e30, jnp.float32).at[flat_ids].max(masked_top)
        shares = flat_mask * masses.reshape(-1) * jnp.exp(masked_top - largest[flat_ids])
        totals = jnp.zeros((total_points,), jnp.float32).at[flat_ids].add(shares)
        norm_log = largest + jnp.log(totals)
        log_rows = norm_log[point_ids]

        def sums_cell(args):
            which_cell, chosen_all, log_all, mask_all = args

            def per_column(carry, items):
                column, chosen, log_column, mask_column = items
                point_rows, scores = scores_of(which_cell, column, chosen)
                weight = jnp.exp(scores - log_column[:, None]) * mask_column[:, None]
                load_sum = carry[1] + jnp.sum(weight, axis=0)
                weighted = carry[0] + jnp.dot(weight.astype(jnp.bfloat16).T, point_rows,
                                              preferred_element_type=jnp.float32)
                return (weighted, load_sum), None

            initial = (jnp.zeros((CENT, D), jnp.float32), jnp.zeros((CENT,), jnp.float32))
            result, unused = lax.scan(per_column, initial, (columns, chosen_all, log_all, mask_all))
            return result

        point_sums, load_sums = lax.map(sums_cell, (cell_ids, picked, log_rows, row_mask))
        new_means = (point_sums + prior_mass * means) / (load_sums[:, :, None] + prior_mass)
        price = price + price_rate * jnp.log((load_sums + prior_mass) / (target + prior_mass))
        means = new_means
    return means, price
```

```python
import functools

import jax
import jax.numpy as jnp
from jax import lax
from jax.experimental import pallas as pl
from jax.experimental.pallas import tpu as pltpu
from jax.sharding import PartitionSpec as P

STEPS = 2
LANES = 128

prior_mass = 1.0
price_rate = 0.5
empty_log = 1e30

VMEM = pl.BlockSpec(memory_space=pltpu.VMEM)


def iota(shape, dim):
    return lax.broadcasted_iota(jnp.int32, shape, dim)


def exact_dot(a, b, dims):
    return lax.dot_general(
        a,
        b,
        (dims, ((), ())),
        precision=lax.Precision.HIGHEST,
        preferred_element_type=jnp.float32,
    )


def small_dot(a, b, dims):
    return lax.dot_general(
        a.astype(jnp.bfloat16),
        b.astype(jnp.bfloat16),
        (dims, ((), ())),
        preferred_element_type=jnp.float32,
    )


def block_names(wanted, cells):
    tops, count = wanted.shape
    cell = iota((cells, count), 0)
    hot = [(wanted[t : t + 1, :] == cell).astype(jnp.float32) for t in range(tops)]
    named = functools.reduce(jnp.add, hot)
    earlier = (iota((count, count), 0) < iota((count, count), 1)).astype(jnp.float32)
    before = small_dot(named, earlier, ((1,), (0,)))
    return hot, named, before


def pack_kernel(cells, capacity, per_block, wanted_ref, points_ref, out_ref):
    wanted = wanted_ref[...]
    count = wanted.shape[1]
    rows = count * per_block
    total = cells * capacity * per_block
    _, named, before = block_names(wanted, cells)
    both = jnp.concatenate([named, before], axis=1)
    chunk = total // 4
    for k in range(4):
        place = iota((chunk, 1), 0) + k * chunk
        owner = (place // (capacity * per_block) == iota((chunk, cells), 1)).astype(jnp.float32)
        spread = small_dot(owner, both, ((1,), (0,)))
        slot = ((place // per_block) % capacity).astype(jnp.float32)
        chosen = spread[:, :count] * (spread[:, count:] == slot).astype(jnp.float32)
        block = iota((chunk, count), 1).astype(jnp.float32)
        source = jnp.sum(chosen * (block + 1.0), axis=1, keepdims=True) - 1.0
        source = source.astype(jnp.int32) * per_block + place % per_block
        pick = (iota((chunk, rows), 1) == source).astype(jnp.float32).astype(jnp.bfloat16)
        moved = jnp.dot(pick, points_ref[...], preferred_element_type=jnp.float32)
        out_ref[k * chunk : (k + 1) * chunk, :] = moved.astype(jnp.bfloat16)


def centre_offset(packed, width):
    return (
        packed[:, width : width + 1].astype(jnp.float32)
        + packed[:, width + 1 : width + 2].astype(jnp.float32)
        + packed[:, width + 2 : width + 3].astype(jnp.float32)
    )


def score_chunk(half, offset, rows):
    return (
        lax.dot_general(half, rows, (((1,), (1,)), ((), ())), preferred_element_type=jnp.float32)
        - offset
    )


def stats_kernel(chunks, packed_ref, incoming_ref, out_ref):
    width = incoming_ref.shape[1]
    packed = packed_ref[...]
    half = packed[:, :width]
    offset = centre_offset(packed, width)
    size = incoming_ref.shape[0] // chunks
    per_owner = out_ref.shape[1]
    part = size // per_owner
    own = iota((part, size), 1) // per_owner == iota((part, size), 0)
    fold = (iota((size, per_owner), 0) % per_owner == iota((size, per_owner), 1)).astype(
        jnp.float32
    )
    for k in range(chunks):
        scores = score_chunk(half, offset, incoming_ref[k * size : (k + 1) * size, :])
        highest = jnp.max(scores, axis=0, keepdims=True)
        mass = jnp.sum(jnp.exp(scores - highest), axis=0, keepdims=True)
        logs = jnp.where(own, highest + jnp.log(mass), 0.0)
        out_ref[k * part : (k + 1) * part, :] = exact_dot(logs, fold, ((1,), (0,)))


def norm_kernel(per_block, capacity, wanted_ref, back_ref, out_ref):
    back = back_ref[...]
    cells = back.shape[0]
    hots, _, before = block_names(wanted_ref[...], cells)
    tops = len(hots)
    count = hots[0].shape[1]
    hot = jnp.concatenate(hots, axis=1)
    slot = small_dot(
        hot * jnp.concatenate([before] * tops, axis=1),
        jnp.ones((cells, capacity * per_block), jnp.float32),
        ((0,), (0,)),
    )
    in_slot = slot == (iota(slot.shape, 1) // per_block).astype(jnp.float32)
    found = jnp.where(in_slot, exact_dot(hot, back, ((0,), (0,))), 0.0)
    part = found[:, :per_block]
    for s in range(1, capacity):
        part = part + found[:, s * per_block : (s + 1) * per_block]
    parts = [part[t * count : (t + 1) * count] for t in range(tops)]
    largest = functools.reduce(jnp.maximum, parts)
    total = functools.reduce(jnp.add, [jnp.exp(part - largest) for part in parts])
    norm = largest + jnp.log(total)
    norm = jnp.concatenate([norm] * capacity, axis=1)
    norm = jnp.where(in_slot, jnp.concatenate([norm] * tops, axis=0), 0.0)
    value = exact_dot(hot, norm, ((1,), (0,)))
    filled = small_dot(hot, in_slot.astype(jnp.float32), ((1,), (0,)))
    out_ref[...] = jnp.where(filled > 0, value, empty_log)


def sums_kernel(chunks, packed_ref, incoming_ref, log_ref, out_ref):
    width = incoming_ref.shape[1]
    packed = packed_ref[...]
    half = packed[:, :width]
    offset = centre_offset(packed, width)
    centres = packed.shape[0]
    size = incoming_ref.shape[0] // chunks
    per_owner = log_ref.shape[1]
    part = size // per_owner
    own = iota((part, size), 1) // per_owner == iota((part, size), 0)
    fold = (iota((per_owner, size), 1) % per_owner == iota((per_owner, size), 0)).astype(
        jnp.float32
    )
    total = jnp.zeros((centres, width), jnp.float32)
    load = jnp.zeros((centres, 1), jnp.float32)
    for k in range(chunks):
        rows = incoming_ref[k * size : (k + 1) * size, :]
        logs = exact_dot(log_ref[k * part : (k + 1) * part, :], fold, ((1,), (0,)))
        logs = jnp.sum(jnp.where(own, logs, 0.0), axis=0, keepdims=True)
        weight = jnp.exp(score_chunk(half, offset, rows) - logs)
        load = load + jnp.sum(weight, axis=1, keepdims=True)
        total = total + jnp.dot(
            weight.astype(jnp.bfloat16), rows, preferred_element_type=jnp.float32
        )
    out_ref[...] = packed_with(total, load)


def packed_with(means, column):
    high = column.astype(jnp.bfloat16)
    rest = column - high.astype(jnp.float32)
    middle = rest.astype(jnp.bfloat16)
    low = (rest - middle.astype(jnp.float32)).astype(jnp.bfloat16)
    lane = iota((means.shape[0], LANES), 1)
    zero = jnp.zeros((means.shape[0], LANES), jnp.bfloat16).astype(jnp.float32)
    tail = jnp.where(
        lane == 0,
        high.astype(jnp.float32),
        jnp.where(
            lane == 1,
            middle.astype(jnp.float32),
            jnp.where(lane == 2, low.astype(jnp.float32), zero),
        ),
    )
    return jnp.concatenate([means.astype(jnp.bfloat16), tail.astype(jnp.bfloat16)], axis=1)


def start_kernel(means_ref, price_ref, out_ref):
    means = means_ref[...]
    offset = 0.5 * jnp.sum(means * means, axis=1, keepdims=True) + price_ref[...]
    out_ref[...] = packed_with(means, offset)


def update_kernel(target, last, sums_ref, means_ref, price_ref, packed_ref, new_ref, cost_ref):
    width = means_ref.shape[1]
    sums = sums_ref[...].astype(jnp.float32)
    total = jnp.sum(sums, axis=0)
    load = total[:, width : width + 1] + total[:, width + 1 : width + 2] + total[:, width + 2 : width + 3]
    means = (total[:, :width] + prior_mass * means_ref[...]) / (load + prior_mass)
    price = price_ref[...] + price_rate * jnp.log((load + prior_mass) / (target + prior_mass))
    new_ref[...] = means
    cost_ref[...] = price
    if last:
        packed_ref[...] = packed_with(means, price)
    else:
        offset = 0.5 * jnp.sum(means * means, axis=1, keepdims=True) + price
        packed_ref[...] = packed_with(means, offset)


def shards(points, candidates, centroids, prices):
    cells = lax.axis_size("row")
    copies = lax.axis_size("col")
    wanted = candidates[0].T
    tops, count = wanted.shape
    width = points.shape[2]
    centres = centroids.shape[1]
    per_block = points.shape[1] // count
    capacity = max(2, (2 * tops * count + cells - 1) // cells)
    slots = capacity * per_block
    rows = cells * slots
    share = centres // copies
    target = copies * count * per_block / centres
    chunks = 4

    outgoing = pl.pallas_call(
        functools.partial(pack_kernel, cells, capacity, per_block),
        out_shape=jax.ShapeDtypeStruct((rows, width), jnp.bfloat16),
        in_specs=[VMEM, VMEM],
        out_specs=VMEM,
        name="pack",
    )(wanted, points[0])
    incoming = lax.all_to_all(outgoing.reshape(cells, slots, width), "row", 0, 0, tiled=True)
    incoming = incoming.reshape(rows, width)

    price_column = prices[0].reshape(centres, 1)
    packed = pl.pallas_call(
        start_kernel,
        out_shape=jax.ShapeDtypeStruct((centres, width + LANES), jnp.bfloat16),
        in_specs=[VMEM, VMEM],
        out_specs=VMEM,
        name="start",
    )(centroids[0], price_column)
    place = lax.axis_index("col") * share
    means = lax.dynamic_slice_in_dim(centroids[0], place, share, 0)
    price = lax.dynamic_slice_in_dim(price_column, place, share, 0)

    def exchanged(values):
        filled = lax.all_to_all(values.reshape(cells, 1, slots), "row", 0, 0, tiled=True)
        return filled.reshape(cells, slots)

    for sweep_index in range(STEPS):
        last = sweep_index == STEPS - 1
        logs = pl.pallas_call(
            functools.partial(stats_kernel, chunks),
            out_shape=jax.ShapeDtypeStruct((cells, slots), jnp.float32),
            in_specs=[VMEM, VMEM],
            out_specs=VMEM,
            name="stats",
        )(packed, incoming)
        slot_log = pl.pallas_call(
            functools.partial(norm_kernel, per_block, capacity),
            out_shape=jax.ShapeDtypeStruct((cells, slots), jnp.float32),
            in_specs=[VMEM, VMEM],
            out_specs=VMEM,
            name="norm",
        )(wanted, exchanged(logs))
        sums = pl.pallas_call(
            functools.partial(sums_kernel, chunks),
            out_shape=jax.ShapeDtypeStruct((centres, width + LANES), jnp.bfloat16),
            in_specs=[VMEM, VMEM, VMEM],
            out_specs=VMEM,
            name="sums",
        )(packed, incoming, exchanged(slot_log))
        pieces = lax.all_to_all(
            sums.reshape(copies, share, width + LANES), "col", 0, 0, tiled=True
        )
        piece, means, price = pl.pallas_call(
            functools.partial(update_kernel, target, last),
            out_shape=(
                jax.ShapeDtypeStruct((share, width + LANES), jnp.bfloat16),
                jax.ShapeDtypeStruct((share, width), jnp.float32),
                jax.ShapeDtypeStruct((share, 1), jnp.float32),
            ),
            in_specs=[VMEM, VMEM, VMEM],
            out_specs=(VMEM, VMEM, VMEM),
            name="update",
        )(pieces, means, price)
        packed = lax.all_gather(piece, "col", axis=0, tiled=True)

    new_centroids = packed[:, :width].astype(jnp.float32)
    new_prices = jnp.sum(packed[:, width : width + 3].astype(jnp.float32), axis=1)
    return (new_centroids[None], new_prices[None])


def solution(mesh):
    placed = (P("col", "row", None), P("col", "row", None), P("row", None, None), P("row", None))
    return jax.shard_map(
        shards,
        mesh=mesh,
        in_specs=placed,
        out_specs=(P("row", None, None), P("row", None)),
        check_vma=False,
    )
```

```python
import functools

import jax
import jax.numpy as jnp
from jax import lax
from jax.experimental import pallas as pl
from jax.experimental.pallas import tpu as pltpu
from jax.sharding import PartitionSpec as P

STEPS = 2
LANES = 128

prior_mass = 1.0
price_rate = 0.5
empty_log = 1e30

VMEM = pl.BlockSpec(memory_space=pltpu.VMEM)


def on_chip(kernel, name, outs, held=None):
    def run(*args):
        marks = held or (True,) * len(args)
        args = [
            pltpu.with_memory_space_constraint(arg, pltpu.VMEM) if mark else arg
            for arg, mark in zip(args, marks)
        ]
        return pl.pallas_call(
            kernel,
            out_shape=outs,
            in_specs=[VMEM] * len(args),
            out_specs=(VMEM,) * len(outs) if isinstance(outs, tuple) else VMEM,
            compiler_params=pltpu.CompilerParams(vmem_limit_bytes=24 << 20),
            name=name,
        )(*args)

    return run


def iota(shape, dim):
    return lax.broadcasted_iota(jnp.int32, shape, dim)


def exact_dot(a, b, dims):
    return lax.dot_general(
        a,
        b,
        (dims, ((), ())),
        precision=lax.Precision.HIGHEST,
        preferred_element_type=jnp.float32,
    )


def small_dot(a, b, dims):
    return lax.dot_general(
        a.astype(jnp.bfloat16),
        b.astype(jnp.bfloat16),
        (dims, ((), ())),
        preferred_element_type=jnp.float32,
    )


def block_names(wanted, cells):
    tops, count = wanted.shape
    cell = iota((cells, count), 0)
    hot = [(wanted[t : t + 1, :] == cell).astype(jnp.float32) for t in range(tops)]
    named = functools.reduce(jnp.add, hot)
    earlier = (iota((count, count), 0) < iota((count, count), 1)).astype(jnp.float32)
    before = small_dot(named, earlier, ((1,), (0,)))
    return hot, named, before


def pack_kernel(cells, capacity, per_block, wanted_ref, points_ref, out_ref):
    wanted = wanted_ref[...]
    count = wanted.shape[1]
    rows = count * per_block
    chunk = out_ref.shape[0]
    _, named, before = block_names(wanted, cells)
    both = jnp.concatenate([named, before], axis=1)
    place = iota((chunk, 1), 0) + pl.program_id(0) * chunk
    owner = (place // (capacity * per_block) == iota((chunk, cells), 1)).astype(jnp.float32)
    spread = small_dot(owner, both, ((1,), (0,)))
    slot = ((place // per_block) % capacity).astype(jnp.float32)
    chosen = spread[:, :count] * (spread[:, count:] == slot).astype(jnp.float32)
    block = iota((chunk, count), 1).astype(jnp.float32)
    source = jnp.sum(chosen * (block + 1.0), axis=1, keepdims=True) - 1.0
    source = source.astype(jnp.int32) * per_block + place % per_block
    pick = (iota((chunk, rows), 1) == source).astype(jnp.float32).astype(jnp.bfloat16)
    moved = jnp.dot(pick, points_ref[...], preferred_element_type=jnp.float32)
    out_ref[...] = moved.astype(jnp.bfloat16)


def centre_offset(packed, width):
    return (
        packed[:, width : width + 1].astype(jnp.float32)
        + packed[:, width + 1 : width + 2].astype(jnp.float32)
        + packed[:, width + 2 : width + 3].astype(jnp.float32)
    )


def score_chunk(half, offset, rows):
    return (
        lax.dot_general(half, rows, (((1,), (1,)), ((), ())), preferred_element_type=jnp.float32)
        - offset
    )


def stats_kernel(chunks, packed_ref, incoming_ref, out_ref):
    width = incoming_ref.shape[1]
    packed = packed_ref[...]
    half = packed[:, :width]
    offset = centre_offset(packed, width)
    size = incoming_ref.shape[0] // chunks
    per_owner = out_ref.shape[1]
    part = size // per_owner
    own = iota((part, size), 1) // per_owner == iota((part, size), 0)
    fold = (iota((size, per_owner), 0) % per_owner == iota((size, per_owner), 1)).astype(
        jnp.float32
    )
    for k in range(chunks):
        scores = score_chunk(half, offset, incoming_ref[k * size : (k + 1) * size, :])
        highest = jnp.max(scores, axis=0, keepdims=True)
        mass = jnp.sum(jnp.exp(scores - highest), axis=0, keepdims=True)
        logs = jnp.where(own, highest + jnp.log(mass), 0.0)
        out_ref[k * part : (k + 1) * part, :] = exact_dot(logs, fold, ((1,), (0,)))


def norm_kernel(per_block, capacity, wanted_ref, back_ref, out_ref):
    back = back_ref[...]
    cells = back.shape[0]
    hots, _, before = block_names(wanted_ref[...], cells)
    tops = len(hots)
    count = hots[0].shape[1]
    hot = jnp.concatenate(hots, axis=1)
    slot = small_dot(
        hot * jnp.concatenate([before] * tops, axis=1),
        jnp.ones((cells, capacity * per_block), jnp.float32),
        ((0,), (0,)),
    )
    in_slot = slot == (iota(slot.shape, 1) // per_block).astype(jnp.float32)
    found = jnp.where(in_slot, exact_dot(hot, back, ((0,), (0,))), 0.0)
    part = found[:, :per_block]
    for s in range(1, capacity):
        part = part + found[:, s * per_block : (s + 1) * per_block]
    parts = [part[t * count : (t + 1) * count] for t in range(tops)]
    largest = functools.reduce(jnp.maximum, parts)
    total = functools.reduce(jnp.add, [jnp.exp(part - largest) for part in parts])
    norm = largest + jnp.log(total)
    norm = jnp.concatenate([norm] * capacity, axis=1)
    norm = jnp.where(in_slot, jnp.concatenate([norm] * tops, axis=0), 0.0)
    value = exact_dot(hot, norm, ((1,), (0,)))
    filled = small_dot(hot, in_slot.astype(jnp.float32), ((1,), (0,)))
    out_ref[...] = jnp.where(filled > 0, value, empty_log)


def sums_kernel(chunks, packed_ref, incoming_ref, log_ref, out_ref):
    width = incoming_ref.shape[1]
    packed = packed_ref[...]
    half = packed[:, :width]
    offset = centre_offset(packed, width)
    centres = packed.shape[0]
    size = incoming_ref.shape[0] // chunks
    per_owner = log_ref.shape[1]
    part = size // per_owner
    own = iota((part, size), 1) // per_owner == iota((part, size), 0)
    fold = (iota((per_owner, size), 1) % per_owner == iota((per_owner, size), 0)).astype(
        jnp.float32
    )
    total = jnp.zeros((centres, width), jnp.float32)
    load = jnp.zeros((centres, 1), jnp.float32)
    for k in range(chunks):
        rows = incoming_ref[k * size : (k + 1) * size, :]
        logs = exact_dot(log_ref[k * part : (k + 1) * part, :], fold, ((1,), (0,)))
        logs = jnp.sum(jnp.where(own, logs, 0.0), axis=0, keepdims=True)
        weight = jnp.exp(score_chunk(half, offset, rows) - logs)
        load = load + jnp.sum(weight, axis=1, keepdims=True)
        total = total + jnp.dot(
            weight.astype(jnp.bfloat16), rows, preferred_element_type=jnp.float32
        )
    out_ref[...] = packed_with(total, load)


def packed_with(means, column):
    high = column.astype(jnp.bfloat16)
    rest = column - high.astype(jnp.float32)
    middle = rest.astype(jnp.bfloat16)
    low = (rest - middle.astype(jnp.float32)).astype(jnp.bfloat16)
    lane = iota((means.shape[0], LANES), 1)
    zero = jnp.zeros((means.shape[0], LANES), jnp.bfloat16).astype(jnp.float32)
    tail = jnp.where(
        lane == 0,
        high.astype(jnp.float32),
        jnp.where(
            lane == 1,
            middle.astype(jnp.float32),
            jnp.where(lane == 2, low.astype(jnp.float32), zero),
        ),
    )
    return jnp.concatenate([means.astype(jnp.bfloat16), tail.astype(jnp.bfloat16)], axis=1)


def start_kernel(means_ref, price_ref, packed_ref, own_ref, cost_ref):
    means = means_ref[...]
    offset = 0.5 * jnp.sum(means * means, axis=1, keepdims=True) + price_ref[...]
    packed_ref[...] = packed_with(means, offset)
    share = own_ref.shape[0]
    place = pl.multiple_of(lax.axis_index("col") * share, share)
    own_ref[...] = means_ref[pl.ds(place, share), :]
    cost_ref[...] = price_ref[pl.ds(place, share), :]


def update_kernel(target, last, sums_ref, means_ref, price_ref, packed_ref, new_ref, cost_ref):
    width = means_ref.shape[1]
    sums = sums_ref[...].astype(jnp.float32)
    total = jnp.sum(sums, axis=0)
    load = total[:, width : width + 1] + total[:, width + 1 : width + 2] + total[:, width + 2 : width + 3]
    means = (total[:, :width] + prior_mass * means_ref[...]) / (load + prior_mass)
    price = price_ref[...] + price_rate * jnp.log((load + prior_mass) / (target + prior_mass))
    new_ref[...] = means
    cost_ref[...] = price
    column = price if last else 0.5 * jnp.sum(means * means, axis=1, keepdims=True) + price
    packed = packed_with(means, column)
    for copy in range(packed_ref.shape[0]):
        packed_ref[copy] = packed


def shards(points, candidates, centroids, prices):
    cells = lax.axis_size("row")
    copies = lax.axis_size("col")
    wanted = candidates[0].T
    tops, count = wanted.shape
    width = points.shape[2]
    centres = centroids.shape[1]
    per_block = points.shape[1] // count
    capacity = max(2, (2 * tops * count + cells - 1) // cells)
    slots = capacity * per_block
    rows = cells * slots
    share = centres // copies
    target = copies * count * per_block / centres
    chunks = 4

    chunk = rows // chunks
    outgoing = pl.pallas_call(
        functools.partial(pack_kernel, cells, capacity, per_block),
        out_shape=jax.ShapeDtypeStruct((rows, width), jnp.bfloat16),
        grid=(chunks,),
        in_specs=[
            pl.BlockSpec(wanted.shape, lambda k: (0, 0)),
            pl.BlockSpec(points.shape[1:], lambda k: (0, 0)),
        ],
        out_specs=pl.BlockSpec((chunk, width), lambda k: (k, 0)),
        name="pack",
    )(wanted, points[0])
    incoming = lax.all_to_all(outgoing.reshape(cells, slots, width), "row", 0, 0, tiled=True)
    incoming = incoming.reshape(rows, width)

    price_column = prices[0].reshape(centres, 1)
    packed, means, price = on_chip(
        start_kernel,
        "start",
        (
            jax.ShapeDtypeStruct((centres, width + LANES), jnp.bfloat16),
            jax.ShapeDtypeStruct((share, width), jnp.float32),
            jax.ShapeDtypeStruct((share, 1), jnp.float32),
        ),
        (False, False),
    )(centroids[0], price_column)

    def exchanged(values):
        filled = lax.all_to_all(values.reshape(cells, 1, slots), "row", 0, 0, tiled=True)
        return filled.reshape(cells, slots)

    for sweep_index in range(STEPS):
        last = sweep_index == STEPS - 1
        logs = on_chip(
            functools.partial(stats_kernel, chunks),
            "stats",
            jax.ShapeDtypeStruct((cells, slots), jnp.float32),
            (sweep_index > 0, True),
        )(packed, incoming)
        slot_log = on_chip(
            functools.partial(norm_kernel, per_block, capacity),
            "norm",
            jax.ShapeDtypeStruct((cells, slots), jnp.float32),
        )(wanted, exchanged(logs))
        sums = on_chip(
            functools.partial(sums_kernel, chunks),
            "sums",
            jax.ShapeDtypeStruct((centres, width + LANES), jnp.bfloat16),
            (sweep_index > 0, True, True),
        )(packed, incoming, exchanged(slot_log))
        pieces = lax.all_to_all(
            sums.reshape(copies, share, width + LANES), "col", 0, 0, tiled=True
        )
        piece, means, price = on_chip(
            functools.partial(update_kernel, target, last),
            "update",
            (
                jax.ShapeDtypeStruct((copies, share, width + LANES), jnp.bfloat16),
                jax.ShapeDtypeStruct((share, width), jnp.float32),
                jax.ShapeDtypeStruct((share, 1), jnp.float32),
            ),
            (True, False, False),
        )(pieces, means, price)
        packed = lax.all_to_all(piece, "col", 0, 0, tiled=True).reshape(centres, width + LANES)

    new_centroids = packed[:, :width].astype(jnp.float32)
    new_prices = jnp.sum(packed[:, width : width + 3].astype(jnp.float32), axis=1)
    return (new_centroids[None], new_prices[None])


def solution(mesh):
    placed = (P("col", "row", None), P("col", "row", None), P("row", None, None), P("row", None))
    return jax.shard_map(
        shards,
        mesh=mesh,
        in_specs=placed,
        out_specs=(P("row", None, None), P("row", None)),
        check_vma=False,
    )
```

```python
import functools

import jax
import jax.numpy as jnp
from jax import lax
from jax.experimental import pallas as pl
from jax.experimental.pallas import tpu as pltpu
from jax.sharding import PartitionSpec as P

STEPS = 2
LANES = 128
PARTS = 4

prior_mass = 1.0
price_rate = 0.5
empty_log = 1e30

VMEM = pl.BlockSpec(memory_space=pltpu.VMEM)


def on_chip(kernel, name, outs, held=None):
    def run(*args):
        marks = held or (True,) * len(args)
        args = [
            pltpu.with_memory_space_constraint(arg, pltpu.VMEM) if mark else arg
            for arg, mark in zip(args, marks)
        ]
        return pl.pallas_call(
            kernel,
            out_shape=outs,
            in_specs=[VMEM] * len(args),
            out_specs=(VMEM,) * len(outs) if isinstance(outs, tuple) else VMEM,
            compiler_params=pltpu.CompilerParams(vmem_limit_bytes=24 << 20),
            name=name,
        )(*args)

    return run


def iota(shape, dim):
    return lax.broadcasted_iota(jnp.int32, shape, dim)


def exact_dot(a, b, dims):
    return lax.dot_general(
        a,
        b,
        (dims, ((), ())),
        precision=lax.Precision.HIGHEST,
        preferred_element_type=jnp.float32,
    )


def small_dot(a, b, dims):
    return lax.dot_general(
        a.astype(jnp.bfloat16),
        b.astype(jnp.bfloat16),
        (dims, ((), ())),
        preferred_element_type=jnp.float32,
    )


def block_names(wanted, cells):
    tops, count = wanted.shape
    cell = iota((cells, count), 0)
    hot = [(wanted[t : t + 1, :] == cell).astype(jnp.float32) for t in range(tops)]
    named = functools.reduce(jnp.add, hot)
    earlier = (iota((count, count), 0) < iota((count, count), 1)).astype(jnp.float32)
    before = small_dot(named, earlier, ((1,), (0,)))
    return hot, named, before


def pack_kernel(cells, capacity, per_block, wanted_ref, points_ref, out_ref, held_ref, sems):
    wanted = wanted_ref[...]
    count = wanted.shape[1]
    rows = count * per_block
    chunks, chunk = held_ref.shape[:2]
    _, named, before = block_names(wanted, cells)
    both = jnp.concatenate([named, before], axis=1)
    copies = []
    for k in range(chunks):
        place = iota((chunk, 1), 0) + k * chunk
        owner = (place // (capacity * per_block) == iota((chunk, cells), 1)).astype(jnp.float32)
        spread = small_dot(owner, both, ((1,), (0,)))
        slot = ((place // per_block) % capacity).astype(jnp.float32)
        chosen = spread[:, :count] * (spread[:, count:] == slot).astype(jnp.float32)
        block = iota((chunk, count), 1).astype(jnp.float32)
        source = jnp.sum(chosen * (block + 1.0), axis=1, keepdims=True) - 1.0
        source = source.astype(jnp.int32) * per_block + place % per_block
        pick = (iota((chunk, rows), 1) == source).astype(jnp.float32).astype(jnp.bfloat16)
        moved = jnp.dot(pick, points_ref[...], preferred_element_type=jnp.float32)
        held_ref[k] = moved.astype(jnp.bfloat16)
        copies.append(
            pltpu.make_async_copy(
                held_ref.at[k], out_ref.at[pl.ds(k * chunk, chunk)], sems.at[k]
            )
        )
        copies[-1].start()
    for copy in copies:
        copy.wait()


def index_kernel(capacity, per_block, tops, names_ref, hot_ref, mask_ref, empty_ref):
    total, lanes = names_ref.shape
    devices = total // PARTS
    count = lanes // tops
    cells = names_ref[pl.ds(1, devices, stride=PARTS), :]
    slots = names_ref[pl.ds(2, devices, stride=PARTS), :]
    mine = cells == lax.axis_index("row").astype(jnp.float32)
    to_block = (iota((lanes, count), 0) % count == iota((lanes, count), 1)).astype(jnp.float32)
    to_top = (iota((lanes, tops), 0) // count == iota((lanes, tops), 1)).astype(jnp.float32)
    found_cells, found_slots, found = [], [], []
    for s in range(capacity):
        at = jnp.where(mine, jnp.where(slots == s, 1.0, 0.0), 0.0)
        block = small_dot(at, to_block, ((1,), (0,)))
        block = jnp.concatenate([block] * tops, axis=1)
        found_cells.append(small_dot(block * cells, to_top, ((1,), (0,))))
        found_slots.append(small_dot(block * slots, to_top, ((1,), (0,))))
        found.append(small_dot(at, jnp.ones((lanes, tops), jnp.float32), ((1,), (0,))))
    table = jnp.concatenate(found_cells + found_slots + found, axis=1)
    span = capacity * tops
    together = LANES // (capacity * per_block)
    size = hot_ref.shape[0]
    step = together * capacity
    row = iota((size, 1), 0)
    inside = (row % step) // capacity
    device = row // (step * tops) * together + inside
    pick = (device == iota((size, devices), 1)).astype(jnp.float32)
    entry = small_dot(pick, table, ((1,), (0,)))
    lane = iota(entry.shape, 1)
    column = (row % capacity) * tops + (row // step) % tops

    def entry_at(start):
        return jnp.sum(jnp.where(lane == start + column, entry, 0.0), axis=1, keepdims=True)

    cell, slot, there = entry_at(0), entry_at(span), entry_at(2 * span) > 0
    spot = iota((size, LANES), 1)
    hot = jnp.where(there, jnp.where(spot.astype(jnp.float32) == cell, 1.0, 0.0), 0.0)
    hot_ref[...] = hot.astype(jnp.bfloat16)
    place = inside * capacity + slot.astype(jnp.int32)
    mask = jnp.where(there, jnp.where(spot // per_block == place, 1.0, 0.0), 0.0)
    mask_ref[...] = mask.astype(jnp.bfloat16)
    full = jnp.where(there, 1.0, 0.0)
    for g in range(size // (step * tops)):
        head = full[g * step * tops : g * step * tops + step]
        empty_ref[g * step : (g + 1) * step, :] = jnp.broadcast_to(1.0 - head, (step, LANES))


def pair_place(at, copies):
    core = lax.axis_index("col") % 2
    half = copies // 2
    return 2 * at + core if at < half else 2 * (at - half) + 1 - core


def centre_offset(packed, width):
    return (
        packed[:, width : width + 1].astype(jnp.float32)
        + packed[:, width + 1 : width + 2].astype(jnp.float32)
        + packed[:, width + 2 : width + 3].astype(jnp.float32)
    )


def score_chunk(half, offset, rows):
    return (
        lax.dot_general(half, rows, (((1,), (1,)), ((), ())), preferred_element_type=jnp.float32)
        - offset
    )


def row_logs(half, offset, rows):
    scores = score_chunk(half, offset, rows)
    highest = jnp.max(scores, axis=0, keepdims=True)
    return highest + jnp.log(jnp.sum(jnp.exp(scores - highest), axis=0, keepdims=True))


def slot_stats_kernel(chunks, packed_ref, incoming_ref, out_ref):
    width = incoming_ref.shape[1]
    packed = packed_ref[...]
    half = packed[:, :width]
    offset = centre_offset(packed, width)
    size = incoming_ref.shape[0] // chunks
    slots = out_ref.shape[1]
    part = size // slots
    for k in range(chunks):
        logs = row_logs(half, offset, incoming_ref[k * size : (k + 1) * size, :])
        for o in range(part):
            out_ref[k * part + o : k * part + o + 1, :] = logs[:, o * slots : (o + 1) * slots]


def norm_kernel(per_block, capacity, wanted_ref, back_ref, out_ref):
    back = back_ref[...]
    cells = back.shape[0]
    wanted = wanted_ref[...]
    hots, _, before = block_names(wanted, cells)
    tops = len(hots)
    count = hots[0].shape[1]
    hot = jnp.concatenate(hots, axis=1)
    slot = small_dot(
        hot * jnp.concatenate([before] * tops, axis=1),
        jnp.ones((cells, capacity * per_block), jnp.float32),
        ((0,), (0,)),
    )
    in_slot = slot == (iota(slot.shape, 1) // per_block).astype(jnp.float32)
    found = jnp.where(in_slot, exact_dot(hot, back, ((0,), (0,))), 0.0)
    part = found[:, :per_block]
    for s in range(1, capacity):
        part = part + found[:, s * per_block : (s + 1) * per_block]
    parts = [part[t * count : (t + 1) * count] for t in range(tops)]
    largest = functools.reduce(jnp.maximum, parts)
    total = functools.reduce(jnp.add, [jnp.exp(part - largest) for part in parts])
    norm = largest + jnp.log(total)
    norm = jnp.concatenate([norm] * capacity, axis=1)
    norm = jnp.where(in_slot, jnp.concatenate([norm] * tops, axis=0), 0.0)
    value = exact_dot(hot, norm, ((1,), (0,)))
    filled = small_dot(hot, in_slot.astype(jnp.float32), ((1,), (0,)))
    value = jnp.where(filled > 0, value, empty_log)
    value = jnp.concatenate([value] * (out_ref.shape[2] // value.shape[1]), axis=1)
    out_ref[:, 0, :] = value
    names = [wanted[t : t + 1, :].astype(jnp.float32) for t in range(tops)]
    places = [jnp.sum(one * before, axis=0, keepdims=True) for one in hots]
    out_ref[:, 1, :] = jnp.broadcast_to(jnp.concatenate(names, axis=1), value.shape)
    out_ref[:, 2, :] = jnp.broadcast_to(jnp.concatenate(places, axis=1), value.shape)
    out_ref[:, 3, :] = jnp.zeros(value.shape, jnp.float32)


def stats_kernel(chunks, mine_ref, other_ref, incoming_ref, out_ref):
    width = incoming_ref.shape[1]
    packed = jnp.concatenate([mine_ref[...], other_ref[...]], axis=0)
    half = packed[:, :width]
    offset = centre_offset(packed, width)
    size = incoming_ref.shape[0] // chunks
    part = size // LANES
    for k in range(chunks):
        logs = row_logs(half, offset, incoming_ref[k * size : (k + 1) * size, :])
        logs = jnp.concatenate(
            [logs[:, i * LANES : (i + 1) * LANES] for i in range(part)], axis=0
        )
        for o in range(out_ref.shape[0]):
            out_ref[o, k * part : (k + 1) * part, :] = logs


def slot_sums_kernel(chunks, per_owner, packed_ref, incoming_ref, log_ref, out_ref):
    width = incoming_ref.shape[1]
    packed = packed_ref[...]
    half = packed[:, :width]
    offset = centre_offset(packed, width)
    centres = packed.shape[0]
    size = incoming_ref.shape[0] // chunks
    part = size // per_owner
    total = jnp.zeros((centres, width), jnp.float32)
    load = jnp.zeros((centres, 1), jnp.float32)
    for k in range(chunks):
        rows = incoming_ref[k * size : (k + 1) * size, :]
        places = [(k * part + o) * PARTS for o in range(part)]
        logs = jnp.concatenate([log_ref[p : p + 1, :per_owner] for p in places], axis=1)
        weight = jnp.exp(score_chunk(half, offset, rows) - logs)
        load = load + jnp.sum(weight, axis=1, keepdims=True)
        total = total + jnp.dot(
            weight.astype(jnp.bfloat16), rows, preferred_element_type=jnp.float32
        )
    out_ref[...] = packed_with(total, load)


def sums_kernel(
    chunks,
    tops,
    per_block,
    mine_ref,
    other_ref,
    incoming_ref,
    logs_ref,
    hot_ref,
    mask_ref,
    empty_ref,
    out_ref,
):
    width = incoming_ref.shape[1]
    packed = jnp.concatenate([mine_ref[...], other_ref[...]], axis=0)
    half = packed[:, :width]
    offset = centre_offset(packed, width)
    centres = packed.shape[0]
    size = incoming_ref.shape[0] // chunks
    part = size // LANES
    groups = incoming_ref.shape[0] // LANES
    cells = logs_ref.shape[0] // groups
    step = empty_ref.shape[0] // groups

    def group_logs(g):
        logs = logs_ref[pl.ds(g, cells, stride=groups), :]
        high = logs.astype(jnp.bfloat16)
        rest = logs - high.astype(jnp.float32)
        middle = rest.astype(jnp.bfloat16)
        low = (rest - middle.astype(jnp.float32)).astype(jnp.bfloat16)
        here = pl.ds(g * step * tops, step * tops)
        found = jnp.dot(
            hot_ref[here, :cells],
            jnp.concatenate([high, middle, low], axis=1),
            preferred_element_type=jnp.float32,
        )
        found = found[:, :LANES] + found[:, LANES : 2 * LANES] + found[:, 2 * LANES :]
        found = jnp.where(mask_ref[here, :].astype(jnp.float32) > 0, found, 0.0)
        shift = per_block
        while shift < LANES:
            found = found + pltpu.roll(found, shift, 1)
            shift *= 2
        parts = [found[t * step : (t + 1) * step] for t in range(tops)]
        largest = functools.reduce(jnp.maximum, parts)
        mass = functools.reduce(jnp.add, [jnp.exp(one - largest) for one in parts])
        norm = largest + jnp.log(mass)
        norm = jnp.where(empty_ref[pl.ds(g * step, step), :] > 0, empty_log, norm)
        own = iota((step, LANES), 0) == iota((step, LANES), 1) // per_block
        return jnp.sum(jnp.where(own, norm, 0.0), axis=0, keepdims=True)

    total = jnp.zeros((centres, width), jnp.float32)
    load = jnp.zeros((centres, 1), jnp.float32)
    for k in range(chunks):
        rows = incoming_ref[k * size : (k + 1) * size, :]
        logs = jnp.concatenate([group_logs(k * part + i) for i in range(part)], axis=1)
        weight = jnp.exp(score_chunk(half, offset, rows) - logs)
        load = load + jnp.sum(weight, axis=1, keepdims=True)
        total = total + jnp.dot(
            weight.astype(jnp.bfloat16), rows, preferred_element_type=jnp.float32
        )
    full = packed_with(total, load)
    share = out_ref.shape[1]
    for at in range(out_ref.shape[0]):
        out_ref[pair_place(at, out_ref.shape[0])] = full[at * share : (at + 1) * share]


def packed_with(means, column):
    high = column.astype(jnp.bfloat16)
    rest = column - high.astype(jnp.float32)
    middle = rest.astype(jnp.bfloat16)
    low = (rest - middle.astype(jnp.float32)).astype(jnp.bfloat16)
    lane = iota((means.shape[0], LANES), 1)
    zero = jnp.zeros((means.shape[0], LANES), jnp.bfloat16).astype(jnp.float32)
    tail = jnp.where(
        lane == 0,
        high.astype(jnp.float32),
        jnp.where(
            lane == 1,
            middle.astype(jnp.float32),
            jnp.where(lane == 2, low.astype(jnp.float32), zero),
        ),
    )
    return jnp.concatenate([means.astype(jnp.bfloat16), tail.astype(jnp.bfloat16)], axis=1)


def start_kernel(means_ref, price_ref, packed_ref, own_ref, cost_ref):
    means = means_ref[...]
    offset = 0.5 * jnp.sum(means * means, axis=1, keepdims=True) + price_ref[...]
    packed_ref[...] = packed_with(means, offset)
    share = own_ref.shape[0]
    place = pl.multiple_of(lax.axis_index("col") * share, share)
    own_ref[...] = means_ref[pl.ds(place, share), :]
    cost_ref[...] = price_ref[pl.ds(place, share), :]


def update_kernel(target, last, sums_ref, means_ref, price_ref, packed_ref, new_ref, cost_ref):
    width = means_ref.shape[1]
    sums = sums_ref[...].astype(jnp.float32)
    total = jnp.sum(sums, axis=0)
    load = total[:, width : width + 1] + total[:, width + 1 : width + 2] + total[:, width + 2 : width + 3]
    means = (total[:, :width] + prior_mass * means_ref[...]) / (load + prior_mass)
    price = price_ref[...] + price_rate * jnp.log((load + prior_mass) / (target + prior_mass))
    new_ref[...] = means
    cost_ref[...] = price
    column = price if last else 0.5 * jnp.sum(means * means, axis=1, keepdims=True) + price
    packed = packed_with(means, column)
    for copy in range(packed_ref.shape[0]):
        packed_ref[copy] = packed


def finish_kernel(mine_ref, other_ref, means_ref, price_ref):
    width = means_ref.shape[1]
    half, share = mine_ref.shape[:2]
    swapped = lax.axis_index("col") % 2 > 0
    for z in range(half):
        mine, other = mine_ref[z].astype(jnp.float32), other_ref[z].astype(jnp.float32)
        for at, part in enumerate(
            (jnp.where(swapped, other, mine), jnp.where(swapped, mine, other))
        ):
            first = (2 * z + at) * share
            means_ref[first : first + share, :] = part[:, :width]
            price = part[:, width : width + 1] + part[:, width + 1 : width + 2]
            price = price + part[:, width + 2 : width + 3]
            here = iota((share, share), 0) == iota((share, share), 1)
            price = jnp.sum(jnp.where(here, price, 0.0), axis=0, keepdims=True)
            price_ref[:, first : first + share] = price


def shards(points, candidates, centroids, prices):
    cells = lax.axis_size("row")
    copies = lax.axis_size("col")
    wanted = candidates[0].T
    tops, count = wanted.shape
    width = points.shape[2]
    centres = centroids.shape[1]
    per_block = points.shape[1] // count
    capacity = max(2, (2 * tops * count + cells - 1) // cells)
    slots = capacity * per_block
    rows = cells * slots
    share = centres // copies
    target = copies * count * per_block / centres
    chunks = 4

    chunk = rows // chunks
    outgoing = pl.pallas_call(
        functools.partial(pack_kernel, cells, capacity, per_block),
        out_shape=jax.ShapeDtypeStruct((rows, width), jnp.bfloat16),
        in_specs=[VMEM, VMEM],
        out_specs=pl.BlockSpec(memory_space=pl.ANY),
        scratch_shapes=[
            pltpu.VMEM((chunks, chunk, width), jnp.bfloat16),
            pltpu.SemaphoreType.DMA((chunks,)),
        ],
        name="pack",
    )(wanted, points[0])
    incoming = lax.all_to_all(outgoing.reshape(cells, slots, width), "row", 0, 0, tiled=True)
    incoming = incoming.reshape(rows, width)

    price_column = prices[0].reshape(centres, 1)
    packed, means, price = on_chip(
        start_kernel,
        "start",
        (
            jax.ShapeDtypeStruct((centres, width + LANES), jnp.bfloat16),
            jax.ShapeDtypeStruct((share, width), jnp.float32),
            jax.ShapeDtypeStruct((share, 1), jnp.float32),
        ),
        (False, False),
    )(centroids[0], price_column)

    sums_shape = jax.ShapeDtypeStruct((centres, width + LANES), jnp.bfloat16)
    for sweep_index in range(STEPS):
        last = sweep_index == STEPS - 1
        if sweep_index == 0:
            logs = on_chip(
                functools.partial(slot_stats_kernel, chunks),
                "stats",
                jax.ShapeDtypeStruct((cells, slots), jnp.float32),
                (False, True),
            )(packed, incoming)
            logs = lax.all_to_all(logs.reshape(cells, 1, slots), "row", 0, 0, tiled=True)
            norms = on_chip(
                functools.partial(norm_kernel, per_block, capacity),
                "norm",
                jax.ShapeDtypeStruct((cells, PARTS, tops * count), jnp.float32),
            )(wanted, logs.reshape(cells, slots))
            norms = lax.all_to_all(norms, "row", 0, 0, tiled=True).reshape(-1, tops * count)
            sums = on_chip(
                functools.partial(slot_sums_kernel, chunks, slots), "sums", sums_shape, (False, True, True)
            )(packed, incoming, norms)
            hot, mask, empty = on_chip(
                functools.partial(index_kernel, capacity, per_block, tops),
                "index",
                (
                    jax.ShapeDtypeStruct((rows // per_block * tops, LANES), jnp.bfloat16),
                    jax.ShapeDtypeStruct((rows // per_block * tops, LANES), jnp.bfloat16),
                    jax.ShapeDtypeStruct((rows // per_block, LANES), jnp.float32),
                ),
            )(norms)
            sums, hot, mask, empty = lax.optimization_barrier((sums, hot, mask, empty))
        else:
            logs = on_chip(
                functools.partial(stats_kernel, chunks),
                "stats_all",
                jax.ShapeDtypeStruct((cells, rows // LANES, LANES), jnp.float32),
            )(mine, other, incoming)
            logs = lax.all_to_all(logs, "row", 0, 0, tiled=True).reshape(-1, LANES)
            sums = on_chip(
                functools.partial(sums_kernel, chunks, tops, per_block),
                "sums_all",
                jax.ShapeDtypeStruct((copies, share, width + LANES), jnp.bfloat16),
            )(mine, other, incoming, logs, hot, mask, empty)
        pieces = lax.all_to_all(
            sums.reshape(copies, share, width + LANES), "col", 0, 0, tiled=True
        )
        half = copies // 2
        piece_shape = (half if last else 1, share, width + LANES)
        piece, means, price = on_chip(
            functools.partial(update_kernel, target, last),
            "update",
            (
                jax.ShapeDtypeStruct(piece_shape, jnp.bfloat16),
                jax.ShapeDtypeStruct((share, width), jnp.float32),
                jax.ShapeDtypeStruct((share, 1), jnp.float32),
            ),
            (True, False, False),
        )(pieces, means, price)
        groups = [list(range(0, copies, 2)), list(range(1, copies, 2))]
        pairs = [(i, i ^ 1) for i in range(copies)]
        if last:
            mine = lax.all_to_all(piece, "col", 0, 0, axis_index_groups=groups, tiled=True)
        else:
            mine = lax.all_gather(piece[0], "col", axis=0, axis_index_groups=groups, tiled=True)
        other = lax.ppermute(mine, "col", pairs)

    new_centroids, new_prices = on_chip(
        finish_kernel,
        "finish",
        (
            jax.ShapeDtypeStruct((centres, width), jnp.float32),
            jax.ShapeDtypeStruct((1, centres), jnp.float32),
        ),
    )(mine, other)
    return (new_centroids[None], new_prices)


def solution(mesh):
    placed = (P("col", "row", None), P("col", "row", None), P("row", None, None), P("row", None))
    return jax.shard_map(
        shards,
        mesh=mesh,
        in_specs=placed,
        out_specs=(P("row", None, None), P("row", None)),
        check_vma=False,
    )
```

```python
import functools

import jax
import jax.numpy as jnp
from jax import lax
from jax.experimental import pallas as pl
from jax.experimental.pallas import tpu as pltpu
from jax.sharding import PartitionSpec as P

STEPS = 2
LANES = 128

prior_mass = 1.0
price_rate = 0.5
empty_log = 1e30

VMEM = pl.BlockSpec(memory_space=pltpu.VMEM)


def on_chip(kernel, name, outs, held=None):
    def run(*args):
        marks = held or (True,) * len(args)
        args = [
            pltpu.with_memory_space_constraint(arg, pltpu.VMEM) if mark else arg
            for arg, mark in zip(args, marks)
        ]
        return pl.pallas_call(
            kernel,
            out_shape=outs,
            in_specs=[VMEM] * len(args),
            out_specs=(VMEM,) * len(outs) if isinstance(outs, tuple) else VMEM,
            compiler_params=pltpu.CompilerParams(vmem_limit_bytes=24 << 20),
            name=name,
        )(*args)

    return run


def iota(shape, dim):
    return lax.broadcasted_iota(jnp.int32, shape, dim)


def small_dot(a, b, dims):
    return lax.dot_general(
        a.astype(jnp.bfloat16),
        b.astype(jnp.bfloat16),
        (dims, ((), ())),
        preferred_element_type=jnp.float32,
    )


def block_names(wanted, cells):
    tops, count = wanted.shape
    cell = iota((cells, count), 0)
    hot = [(wanted[t : t + 1, :] == cell).astype(jnp.float32) for t in range(tops)]
    named = functools.reduce(jnp.add, hot)
    earlier = (iota((count, count), 0) < iota((count, count), 1)).astype(jnp.float32)
    before = small_dot(named, earlier, ((1,), (0,)))
    return hot, named, before


def pack_kernel(cells, capacity, per_block, wanted_ref, points_ref, out_ref, held_ref, sems):
    wanted = wanted_ref[...]
    count = wanted.shape[1]
    rows = count * per_block
    chunks, chunk = held_ref.shape[:2]
    _, named, before = block_names(wanted, cells)
    both = jnp.concatenate([named, before], axis=1)
    copies = []
    for k in range(chunks):
        place = iota((chunk, 1), 0) + k * chunk
        owner = (place // (capacity * per_block) == iota((chunk, cells), 1)).astype(jnp.float32)
        spread = small_dot(owner, both, ((1,), (0,)))
        slot = ((place // per_block) % capacity).astype(jnp.float32)
        chosen = spread[:, :count] * (spread[:, count:] == slot).astype(jnp.float32)
        block = iota((chunk, count), 1).astype(jnp.float32)
        source = jnp.sum(chosen * (block + 1.0), axis=1, keepdims=True) - 1.0
        source = source.astype(jnp.int32) * per_block + place % per_block
        pick = (iota((chunk, rows), 1) == source).astype(jnp.float32).astype(jnp.bfloat16)
        moved = jnp.dot(pick, points_ref[...], preferred_element_type=jnp.float32)
        held_ref[k] = moved.astype(jnp.bfloat16)
        copies.append(
            pltpu.make_async_copy(
                held_ref.at[k], out_ref.at[pl.ds(k * chunk, chunk)], sems.at[k]
            )
        )
        copies[-1].start()
    for copy in copies:
        copy.wait()


def index_kernel(capacity, per_block, tops, held_ref, hot_ref, mask_ref, empty_ref):
    lanes = held_ref.shape[1]
    groups = empty_ref.shape[0] * per_block // LANES
    sent = groups + 2
    devices = held_ref.shape[0] // sent
    count = lanes // tops
    cells = held_ref[pl.ds(groups, devices, stride=sent), :]
    slots = held_ref[pl.ds(groups + 1, devices, stride=sent), :]
    mine = cells == lax.axis_index("row").astype(jnp.float32)
    to_block = (iota((lanes, count), 0) % count == iota((lanes, count), 1)).astype(jnp.float32)
    to_top = (iota((lanes, tops), 0) // count == iota((lanes, tops), 1)).astype(jnp.float32)
    found_cells, found_slots, found = [], [], []
    for s in range(capacity):
        at = jnp.where(mine, jnp.where(slots == s, 1.0, 0.0), 0.0)
        block = small_dot(at, to_block, ((1,), (0,)))
        block = jnp.concatenate([block] * tops, axis=1)
        found_cells.append(small_dot(block * cells, to_top, ((1,), (0,))))
        found_slots.append(small_dot(block * slots, to_top, ((1,), (0,))))
        found.append(small_dot(at, jnp.ones((lanes, tops), jnp.float32), ((1,), (0,))))
    table = jnp.concatenate(found_cells + found_slots + found, axis=1)
    span = capacity * tops
    together = LANES // (capacity * per_block)
    size = hot_ref.shape[0]
    step = together * capacity
    row = iota((size, 1), 0)
    inside = (row % step) // capacity
    device = row // (step * tops) * together + inside
    pick = (device == iota((size, devices), 1)).astype(jnp.float32)
    entry = small_dot(pick, table, ((1,), (0,)))
    lane = iota(entry.shape, 1)
    column = (row % capacity) * tops + (row // step) % tops

    def entry_at(start):
        return jnp.sum(jnp.where(lane == start + column, entry, 0.0), axis=1, keepdims=True)

    cell, slot, there = entry_at(0), entry_at(span), entry_at(2 * span) > 0
    spot = iota((size, LANES), 1)
    hot = jnp.where(there, jnp.where(spot.astype(jnp.float32) == cell, 1.0, 0.0), 0.0)
    hot_ref[...] = hot.astype(jnp.bfloat16)
    place = inside * capacity + slot.astype(jnp.int32)
    mask = jnp.where(there, jnp.where(spot // per_block == place, 1.0, 0.0), 0.0)
    mask_ref[...] = mask.astype(jnp.bfloat16)
    full = jnp.where(there, 1.0, 0.0)
    for g in range(size // (step * tops)):
        head = full[g * step * tops : g * step * tops + step]
        empty_ref[g * step : (g + 1) * step, :] = jnp.broadcast_to(1.0 - head, (step, LANES))


def centre_offset(packed, width):
    return (
        packed[:, width : width + 1].astype(jnp.float32)
        + packed[:, width + 1 : width + 2].astype(jnp.float32)
        + packed[:, width + 2 : width + 3].astype(jnp.float32)
    )


def score_chunk(half, offset, rows):
    return (
        lax.dot_general(half, rows, (((1,), (1,)), ((), ())), preferred_element_type=jnp.float32)
        - offset
    )


def row_logs(half, offset, rows):
    scores = score_chunk(half, offset, rows)
    highest = jnp.max(scores, axis=0, keepdims=True)
    return highest + jnp.log(jnp.sum(jnp.exp(scores - highest), axis=0, keepdims=True))


def stats_kernel(chunks, cells, packed_ref, incoming_ref, *refs):
    names_ref, out_ref = refs if len(refs) > 1 else (None, refs[0])
    width = incoming_ref.shape[1]
    packed = packed_ref[...]
    half = packed[:, :width]
    offset = centre_offset(packed, width)
    size = incoming_ref.shape[0] // chunks
    part = size // LANES
    sent = out_ref.shape[0] // cells
    for k in range(chunks):
        logs = row_logs(half, offset, incoming_ref[k * size : (k + 1) * size, :])
        logs = jnp.concatenate(
            [logs[:, i * LANES : (i + 1) * LANES] for i in range(part)], axis=0
        )
        for o in range(cells):
            out_ref[o * sent + k * part : o * sent + (k + 1) * part, :] = logs
    if names_ref is not None:
        for o in range(cells):
            out_ref[(o + 1) * sent - 2 : (o + 1) * sent, :] = names_ref[...]


def sums_kernel(
    chunks,
    tops,
    per_block,
    cells,
    packed_ref,
    incoming_ref,
    logs_ref,
    hot_ref,
    mask_ref,
    empty_ref,
    out_ref,
):
    width = incoming_ref.shape[1]
    packed = packed_ref[...]
    half = packed[:, :width]
    offset = centre_offset(packed, width)
    centres = packed.shape[0]
    size = incoming_ref.shape[0] // chunks
    part = size // LANES
    groups = incoming_ref.shape[0] // LANES
    sent = logs_ref.shape[0] // cells
    step = empty_ref.shape[0] // groups

    def group_logs(g):
        logs = logs_ref[pl.ds(g, cells, stride=sent), :]
        high = logs.astype(jnp.bfloat16)
        rest = logs - high.astype(jnp.float32)
        middle = rest.astype(jnp.bfloat16)
        low = (rest - middle.astype(jnp.float32)).astype(jnp.bfloat16)
        here = pl.ds(g * step * tops, step * tops)
        found = jnp.dot(
            hot_ref[here, :cells],
            jnp.concatenate([high, middle, low], axis=1),
            preferred_element_type=jnp.float32,
        )
        found = found[:, :LANES] + found[:, LANES : 2 * LANES] + found[:, 2 * LANES :]
        found = jnp.where(mask_ref[here, :].astype(jnp.float32) > 0, found, 0.0)
        shift = per_block
        while shift < LANES:
            found = found + pltpu.roll(found, shift, 1)
            shift *= 2
        parts = [found[t * step : (t + 1) * step] for t in range(tops)]
        largest = functools.reduce(jnp.maximum, parts)
        mass = functools.reduce(jnp.add, [jnp.exp(one - largest) for one in parts])
        norm = largest + jnp.log(mass)
        norm = jnp.where(empty_ref[pl.ds(g * step, step), :] > 0, empty_log, norm)
        own = iota((step, LANES), 0) == iota((step, LANES), 1) // per_block
        return jnp.sum(jnp.where(own, norm, 0.0), axis=0, keepdims=True)

    total = jnp.zeros((centres, width), jnp.float32)
    load = jnp.zeros((centres, 1), jnp.float32)
    for k in range(chunks):
        rows = incoming_ref[k * size : (k + 1) * size, :]
        logs = jnp.concatenate([group_logs(k * part + i) for i in range(part)], axis=1)
        weight = jnp.exp(score_chunk(half, offset, rows) - logs)
        load = load + jnp.sum(weight, axis=1, keepdims=True)
        total = total + jnp.dot(
            weight.astype(jnp.bfloat16), rows, preferred_element_type=jnp.float32
        )
    out_ref[...] = packed_with(total, load)


def packed_with(means, column):
    high = column.astype(jnp.bfloat16)
    rest = column - high.astype(jnp.float32)
    middle = rest.astype(jnp.bfloat16)
    low = (rest - middle.astype(jnp.float32)).astype(jnp.bfloat16)
    lane = iota((means.shape[0], LANES), 1)
    zero = jnp.zeros((means.shape[0], LANES), jnp.bfloat16).astype(jnp.float32)
    tail = jnp.where(
        lane == 0,
        high.astype(jnp.float32),
        jnp.where(
            lane == 1,
            middle.astype(jnp.float32),
            jnp.where(lane == 2, low.astype(jnp.float32), zero),
        ),
    )
    return jnp.concatenate([means.astype(jnp.bfloat16), tail.astype(jnp.bfloat16)], axis=1)


def start_kernel(cells, wanted_ref, means_ref, price_ref, packed_ref, own_ref, cost_ref, names_ref):
    means = means_ref[...]
    offset = 0.5 * jnp.sum(means * means, axis=1, keepdims=True) + price_ref[...]
    packed_ref[...] = packed_with(means, offset)
    share = own_ref.shape[0]
    place = pl.multiple_of(lax.axis_index("col") * share, share)
    own_ref[...] = means_ref[pl.ds(place, share), :]
    cost_ref[...] = price_ref[pl.ds(place, share), :]
    wanted = wanted_ref[...]
    hots, _, before = block_names(wanted, cells)
    names = [wanted[t : t + 1, :].astype(jnp.float32) for t in range(len(hots))]
    places = [jnp.sum(hot * before, axis=0, keepdims=True) for hot in hots]
    names_ref[0:1, :] = jnp.concatenate(names, axis=1)
    names_ref[1:2, :] = jnp.concatenate(places, axis=1)


def update_kernel(target, last, sums_ref, means_ref, price_ref, packed_ref, new_ref, cost_ref):
    width = means_ref.shape[1]
    sums = sums_ref[...].astype(jnp.float32)
    total = jnp.sum(sums, axis=0)
    load = total[:, width : width + 1] + total[:, width + 1 : width + 2] + total[:, width + 2 : width + 3]
    means = (total[:, :width] + prior_mass * means_ref[...]) / (load + prior_mass)
    price = price_ref[...] + price_rate * jnp.log((load + prior_mass) / (target + prior_mass))
    new_ref[...] = means
    cost_ref[...] = price
    column = price if last else 0.5 * jnp.sum(means * means, axis=1, keepdims=True) + price
    packed = packed_with(means, column)
    for copy in range(packed_ref.shape[0]):
        packed_ref[copy] = packed


def finish_kernel(packed_ref, means_ref, price_ref):
    width = means_ref.shape[1]
    packed = packed_ref[...]
    means_ref[...] = packed[:, :width].astype(jnp.float32)
    price = centre_offset(packed, width)
    count = packed.shape[0]
    here = iota((count, count), 0) == iota((count, count), 1)
    price_ref[...] = jnp.sum(jnp.where(here, price, 0.0), axis=0, keepdims=True)


def shards(points, candidates, centroids, prices):
    cells = lax.axis_size("row")
    copies = lax.axis_size("col")
    wanted = candidates[0].T
    tops, count = wanted.shape
    width = points.shape[2]
    centres = centroids.shape[1]
    per_block = points.shape[1] // count
    capacity = max(2, (2 * tops * count + cells - 1) // cells)
    slots = capacity * per_block
    rows = cells * slots
    share = centres // copies
    target = copies * count * per_block / centres
    chunks = 4

    chunk = rows // chunks
    outgoing = pl.pallas_call(
        functools.partial(pack_kernel, cells, capacity, per_block),
        out_shape=jax.ShapeDtypeStruct((rows, width), jnp.bfloat16),
        in_specs=[VMEM, VMEM],
        out_specs=pl.BlockSpec(memory_space=pl.ANY),
        scratch_shapes=[
            pltpu.VMEM((chunks, chunk, width), jnp.bfloat16),
            pltpu.SemaphoreType.DMA((chunks,)),
        ],
        name="pack",
    )(wanted, points[0])
    incoming = lax.all_to_all(outgoing.reshape(cells, slots, width), "row", 0, 0, tiled=True)
    incoming = incoming.reshape(rows, width)

    price_column = prices[0].reshape(centres, 1)
    packed, means, price, names = on_chip(
        functools.partial(start_kernel, cells),
        "start",
        (
            jax.ShapeDtypeStruct((centres, width + LANES), jnp.bfloat16),
            jax.ShapeDtypeStruct((share, width), jnp.float32),
            jax.ShapeDtypeStruct((share, 1), jnp.float32),
            jax.ShapeDtypeStruct((2, tops * count), jnp.float32),
        ),
        (False, False, False),
    )(wanted, centroids[0], price_column)

    groups = rows // LANES
    for sweep_index in range(STEPS):
        last = sweep_index == STEPS - 1
        first = sweep_index == 0
        sent = groups + 2 if first else groups
        logs = on_chip(
            functools.partial(stats_kernel, chunks, cells),
            "stats",
            jax.ShapeDtypeStruct((cells * sent, LANES), jnp.float32),
            (False, True, False) if first else None,
        )(packed, incoming, *((names,) if first else ()))
        logs = logs.reshape(cells, sent // 2, 2, LANES)
        logs = lax.all_to_all(logs, "row", 0, 0, tiled=True).reshape(cells * sent, LANES)
        if first:
            lines = rows // per_block
            hot, mask, empty = on_chip(
                functools.partial(index_kernel, capacity, per_block, tops),
                "index",
                (
                    jax.ShapeDtypeStruct((lines * tops, LANES), jnp.bfloat16),
                    jax.ShapeDtypeStruct((lines * tops, LANES), jnp.bfloat16),
                    jax.ShapeDtypeStruct((lines, LANES), jnp.float32),
                ),
            )(logs)
        sums = on_chip(
            functools.partial(sums_kernel, chunks, tops, per_block, cells),
            "sums",
            jax.ShapeDtypeStruct((centres, width + LANES), jnp.bfloat16),
            (False,) + (True,) * 5 if first else None,
        )(packed, incoming, logs, hot, mask, empty)
        pieces = lax.all_to_all(
            sums.reshape(copies, share, width + LANES), "col", 0, 0, tiled=True
        )
        piece, means, price = on_chip(
            functools.partial(update_kernel, target, last),
            "update",
            (
                jax.ShapeDtypeStruct((copies, share, width + LANES), jnp.bfloat16),
                jax.ShapeDtypeStruct((share, width), jnp.float32),
                jax.ShapeDtypeStruct((share, 1), jnp.float32),
            ),
            (True, False, False),
        )(pieces, means, price)
        packed = lax.all_to_all(piece, "col", 0, 0, tiled=True).reshape(centres, width + LANES)

    new_centroids, new_prices = on_chip(
        finish_kernel,
        "finish",
        (
            jax.ShapeDtypeStruct((centres, width), jnp.float32),
            jax.ShapeDtypeStruct((1, centres), jnp.float32),
        ),
    )(packed)
    return (new_centroids[None], new_prices)


def solution(mesh):
    placed = (P("col", "row", None), P("col", "row", None), P("row", None, None), P("row", None))
    return jax.shard_map(
        shards,
        mesh=mesh,
        in_specs=placed,
        out_specs=(P("row", None, None), P("row", None)),
        check_vma=False,
    )
```

```python
import functools

import jax
import jax.numpy as jnp
from jax import lax
from jax.experimental import pallas as pl
from jax.experimental.pallas import tpu as pltpu
from jax.sharding import PartitionSpec as P

STEPS = 2
LANES = 128
EXTRA = 8

prior_mass = 1.0
price_rate = 0.5
empty_log = 1e30

VMEM = pl.BlockSpec(memory_space=pltpu.VMEM)


def on_chip(kernel, name, outs, held=None):
    def run(*args):
        marks = held or (True,) * len(args)
        args = [
            pltpu.with_memory_space_constraint(arg, pltpu.VMEM) if mark else arg
            for arg, mark in zip(args, marks)
        ]
        return pl.pallas_call(
            kernel,
            out_shape=outs,
            in_specs=[VMEM] * len(args),
            out_specs=(VMEM,) * len(outs) if isinstance(outs, tuple) else VMEM,
            compiler_params=pltpu.CompilerParams(vmem_limit_bytes=24 << 20),
            name=name,
        )(*args)

    return run


def iota(shape, dim):
    return lax.broadcasted_iota(jnp.int32, shape, dim)


def small_dot(a, b, dims):
    return lax.dot_general(
        a.astype(jnp.bfloat16),
        b.astype(jnp.bfloat16),
        (dims, ((), ())),
        preferred_element_type=jnp.float32,
    )


def block_names(wanted, cells):
    tops, count = wanted.shape
    cell = iota((cells, count), 0)
    hot = [(wanted[t : t + 1, :] == cell).astype(jnp.float32) for t in range(tops)]
    named = functools.reduce(jnp.add, hot)
    earlier = (iota((count, count), 0) < iota((count, count), 1)).astype(jnp.float32)
    before = small_dot(named, earlier, ((1,), (0,)))
    return hot, named, before


def pack_kernel(cells, capacity, per_block, wanted_ref, points_ref, out_ref, held_ref, sems):
    wanted = wanted_ref[...]
    count = wanted.shape[1]
    rows = count * per_block
    chunks, chunk = held_ref.shape[:2]
    _, named, before = block_names(wanted, cells)
    both = jnp.concatenate([named, before], axis=1)
    copies = []
    for k in range(chunks):
        place = iota((chunk, 1), 0) + k * chunk
        owner = (place // (capacity * per_block) == iota((chunk, cells), 1)).astype(jnp.float32)
        spread = small_dot(owner, both, ((1,), (0,)))
        slot = ((place // per_block) % capacity).astype(jnp.float32)
        chosen = spread[:, :count] * (spread[:, count:] == slot).astype(jnp.float32)
        block = iota((chunk, count), 1).astype(jnp.float32)
        source = jnp.sum(chosen * (block + 1.0), axis=1, keepdims=True) - 1.0
        source = source.astype(jnp.int32) * per_block + place % per_block
        pick = (iota((chunk, rows), 1) == source).astype(jnp.float32).astype(jnp.bfloat16)
        moved = jnp.dot(pick, points_ref[...], preferred_element_type=jnp.float32)
        held_ref[k] = moved.astype(jnp.bfloat16)
        copies.append(
            pltpu.make_async_copy(
                held_ref.at[k], out_ref.at[pl.ds(k * chunk, chunk)], sems.at[k]
            )
        )
        copies[-1].start()
    for copy in copies:
        copy.wait()


def index_kernel(capacity, per_block, tops, held_ref, hot_ref, mask_ref, empty_ref):
    lanes = held_ref.shape[1]
    groups = empty_ref.shape[0] * per_block // LANES
    sent = groups + 2
    devices = held_ref.shape[0] // sent
    count = lanes // tops
    cells = held_ref[pl.ds(groups, devices, stride=sent), :]
    slots = held_ref[pl.ds(groups + 1, devices, stride=sent), :]
    mine = cells == lax.axis_index("row").astype(jnp.float32)
    to_block = (iota((lanes, count), 0) % count == iota((lanes, count), 1)).astype(jnp.float32)
    to_top = (iota((lanes, tops), 0) // count == iota((lanes, tops), 1)).astype(jnp.float32)
    found_cells, found_slots, found = [], [], []
    for s in range(capacity):
        at = jnp.where(mine, jnp.where(slots == s, 1.0, 0.0), 0.0)
        block = small_dot(at, to_block, ((1,), (0,)))
        block = jnp.concatenate([block] * tops, axis=1)
        found_cells.append(small_dot(block * cells, to_top, ((1,), (0,))))
        found_slots.append(small_dot(block * slots, to_top, ((1,), (0,))))
        found.append(small_dot(at, jnp.ones((lanes, tops), jnp.float32), ((1,), (0,))))
    table = jnp.concatenate(found_cells + found_slots + found, axis=1)
    span = capacity * tops
    together = LANES // (capacity * per_block)
    size = hot_ref.shape[0]
    step = together * capacity
    row = iota((size, 1), 0)
    inside = (row % step) // capacity
    device = row // (step * tops) * together + inside
    pick = (device == iota((size, devices), 1)).astype(jnp.float32)
    entry = small_dot(pick, table, ((1,), (0,)))
    lane = iota(entry.shape, 1)
    column = (row % capacity) * tops + (row // step) % tops

    def entry_at(start):
        return jnp.sum(jnp.where(lane == start + column, entry, 0.0), axis=1, keepdims=True)

    cell, slot, there = entry_at(0), entry_at(span), entry_at(2 * span) > 0
    spot = iota((size, LANES), 1)
    hot = jnp.where(there, jnp.where(spot.astype(jnp.float32) == cell, 1.0, 0.0), 0.0)
    hot_ref[...] = hot.astype(jnp.bfloat16)
    place = inside * capacity + slot.astype(jnp.int32)
    mask = jnp.where(there, jnp.where(spot // per_block == place, 1.0, 0.0), 0.0)
    mask_ref[...] = mask.astype(jnp.bfloat16)
    full = jnp.where(there, 1.0, 0.0)
    for g in range(size // (step * tops)):
        head = full[g * step * tops : g * step * tops + step]
        empty_ref[g * step : (g + 1) * step, :] = jnp.broadcast_to(1.0 - head, (step, LANES))


def share_rows(share, width):
    return width // LANES * share + EXTRA


def store_share(ref, first, means, column):
    share, width = means.shape
    for tile in range(width // LANES):
        at = first + tile * share
        ref[at : at + share, :] = means[:, tile * LANES : (tile + 1) * LANES].astype(jnp.bfloat16)
    line = jnp.sum(
        jnp.where(iota((share, LANES), 0) == iota((share, LANES), 1), column, 0.0),
        axis=0,
        keepdims=True,
    )
    high = line.astype(jnp.bfloat16).astype(jnp.float32)
    middle = (line - high).astype(jnp.bfloat16).astype(jnp.float32)
    low = line - high - middle
    row = iota((EXTRA, LANES), 0)
    tail = jnp.where(
        row == 0, high, jnp.where(row == 1, middle, jnp.where(row == 2, low, 0.0))
    )
    at = first + width // LANES * share
    ref[at : at + EXTRA, :] = tail.astype(jnp.bfloat16)


def load_column(tail, share):
    line = tail[0:1, :] + tail[1:2, :] + tail[2:3, :]
    here = iota((share, LANES), 0) == iota((share, LANES), 1)
    return jnp.sum(jnp.where(here, line, 0.0), axis=1, keepdims=True)


def load_shares(ref, share, width):
    tiles = width // LANES
    size = share_rows(share, width)
    firsts = [o * size for o in range(ref.shape[0] // size)]
    means = jnp.concatenate(
        [
            jnp.concatenate(
                [ref[f + t * share : f + (t + 1) * share, :] for f in firsts], axis=0
            )
            for t in range(tiles)
        ],
        axis=1,
    )
    column = jnp.concatenate(
        [
            load_column(ref[f + size - EXTRA : f + size, :].astype(jnp.float32), share)
            for f in firsts
        ],
        axis=0,
    )
    return means, column


def score_chunk(half, offset, rows):
    return (
        lax.dot_general(half, rows, (((1,), (1,)), ((), ())), preferred_element_type=jnp.float32)
        - offset
    )


def row_logs(half, offset, rows):
    scores = score_chunk(half, offset, rows)
    highest = jnp.max(scores, axis=0, keepdims=True)
    return highest + jnp.log(jnp.sum(jnp.exp(scores - highest), axis=0, keepdims=True))


def stats_kernel(chunks, cells, share, packed_ref, incoming_ref, *refs):
    names_ref, out_ref = refs if len(refs) > 1 else (None, refs[0])
    width = incoming_ref.shape[1]
    half, offset = load_shares(packed_ref, share, width)
    size = incoming_ref.shape[0] // chunks
    part = size // LANES
    sent = out_ref.shape[0] // cells
    for k in range(chunks):
        logs = row_logs(half, offset, incoming_ref[k * size : (k + 1) * size, :])
        logs = jnp.concatenate(
            [logs[:, i * LANES : (i + 1) * LANES] for i in range(part)], axis=0
        )
        for o in range(cells):
            out_ref[o * sent + k * part : o * sent + (k + 1) * part, :] = logs
    if names_ref is not None:
        for o in range(cells):
            out_ref[(o + 1) * sent - 2 : (o + 1) * sent, :] = names_ref[...]


def sums_kernel(
    chunks,
    tops,
    per_block,
    cells,
    share,
    packed_ref,
    incoming_ref,
    logs_ref,
    hot_ref,
    mask_ref,
    empty_ref,
    out_ref,
):
    width = incoming_ref.shape[1]
    half, offset = load_shares(packed_ref, share, width)
    centres = half.shape[0]
    size = incoming_ref.shape[0] // chunks
    part = size // LANES
    groups = incoming_ref.shape[0] // LANES
    sent = logs_ref.shape[0] // cells
    step = empty_ref.shape[0] // groups

    def group_logs(g):
        logs = logs_ref[pl.ds(g, cells, stride=sent), :]
        high = logs.astype(jnp.bfloat16)
        rest = logs - high.astype(jnp.float32)
        middle = rest.astype(jnp.bfloat16)
        low = (rest - middle.astype(jnp.float32)).astype(jnp.bfloat16)
        here = pl.ds(g * step * tops, step * tops)
        found = jnp.dot(
            hot_ref[here, :cells],
            jnp.concatenate([high, middle, low], axis=1),
            preferred_element_type=jnp.float32,
        )
        found = found[:, :LANES] + found[:, LANES : 2 * LANES] + found[:, 2 * LANES :]
        found = jnp.where(mask_ref[here, :].astype(jnp.float32) > 0, found, 0.0)
        shift = per_block
        while shift < LANES:
            found = found + pltpu.roll(found, shift, 1)
            shift *= 2
        parts = [found[t * step : (t + 1) * step] for t in range(tops)]
        largest = functools.reduce(jnp.maximum, parts)
        mass = functools.reduce(jnp.add, [jnp.exp(one - largest) for one in parts])
        norm = largest + jnp.log(mass)
        norm = jnp.where(empty_ref[pl.ds(g * step, step), :] > 0, empty_log, norm)
        own = iota((step, LANES), 0) == iota((step, LANES), 1) // per_block
        return jnp.sum(jnp.where(own, norm, 0.0), axis=0, keepdims=True)

    total = jnp.zeros((centres, width), jnp.float32)
    load = jnp.zeros((centres, 1), jnp.float32)
    for k in range(chunks):
        rows = incoming_ref[k * size : (k + 1) * size, :]
        logs = jnp.concatenate([group_logs(k * part + i) for i in range(part)], axis=1)
        weight = jnp.exp(score_chunk(half, offset, rows) - logs)
        load = load + jnp.sum(weight, axis=1, keepdims=True)
        total = total + jnp.dot(
            weight.astype(jnp.bfloat16), rows, preferred_element_type=jnp.float32
        )
    for o in range(centres // share):
        here = slice(o * share, (o + 1) * share)
        store_share(out_ref, o * share_rows(share, width), total[here], load[here])


def start_kernel(cells, wanted_ref, means_ref, price_ref, packed_ref, own_ref, cost_ref, names_ref):
    means = means_ref[...]
    offset = 0.5 * jnp.sum(means * means, axis=1, keepdims=True) + price_ref[...]
    share, width = own_ref.shape
    for o in range(means.shape[0] // share):
        here = slice(o * share, (o + 1) * share)
        store_share(packed_ref, o * share_rows(share, width), means[here], offset[here])
    place = pl.multiple_of(lax.axis_index("col") * share, share)
    own_ref[...] = means_ref[pl.ds(place, share), :]
    cost_ref[...] = price_ref[pl.ds(place, share), :]
    wanted = wanted_ref[...]
    hots, _, before = block_names(wanted, cells)
    names = [wanted[t : t + 1, :].astype(jnp.float32) for t in range(len(hots))]
    places = [jnp.sum(hot * before, axis=0, keepdims=True) for hot in hots]
    names_ref[0:1, :] = jnp.concatenate(names, axis=1)
    names_ref[1:2, :] = jnp.concatenate(places, axis=1)


def update_kernel(target, last, sums_ref, means_ref, price_ref, packed_ref, new_ref, cost_ref):
    share, width = means_ref.shape
    size = share_rows(share, width)
    copies = sums_ref.shape[0] // size
    total = sums_ref[0:size, :].astype(jnp.float32)
    for copy in range(1, copies):
        total = total + sums_ref[copy * size : (copy + 1) * size, :].astype(jnp.float32)
    load = load_column(total[size - EXTRA :], share)
    tiles = [total[t * share : (t + 1) * share] for t in range(width // LANES)]
    total = jnp.concatenate(tiles, axis=1)
    means = (total + prior_mass * means_ref[...]) / (load + prior_mass)
    price = price_ref[...] + price_rate * jnp.log((load + prior_mass) / (target + prior_mass))
    new_ref[...] = means
    cost_ref[...] = price
    column = price if last else 0.5 * jnp.sum(means * means, axis=1, keepdims=True) + price
    store_share(packed_ref, 0, means, column)
    packed = packed_ref[0:size, :]
    for copy in range(1, copies):
        packed_ref[copy * size : (copy + 1) * size, :] = packed


def finish_kernel(share, packed_ref, means_ref, price_ref):
    means, price = load_shares(packed_ref, share, means_ref.shape[1])
    means_ref[...] = means.astype(jnp.float32)
    count = means.shape[0]
    here = iota((count, count), 0) == iota((count, count), 1)
    price_ref[...] = jnp.sum(jnp.where(here, price, 0.0), axis=0, keepdims=True)


def shards(points, candidates, centroids, prices):
    cells = lax.axis_size("row")
    copies = lax.axis_size("col")
    wanted = candidates[0].T
    tops, count = wanted.shape
    width = points.shape[2]
    centres = centroids.shape[1]
    per_block = points.shape[1] // count
    capacity = max(2, (2 * tops * count + cells - 1) // cells)
    slots = capacity * per_block
    rows = cells * slots
    share = centres // copies
    target = copies * count * per_block / centres
    chunks = 4
    size = share_rows(share, width)
    packed_shape = jax.ShapeDtypeStruct((copies * size, LANES), jnp.bfloat16)

    chunk = rows // chunks
    outgoing = pl.pallas_call(
        functools.partial(pack_kernel, cells, capacity, per_block),
        out_shape=jax.ShapeDtypeStruct((rows, width), jnp.bfloat16),
        in_specs=[VMEM, VMEM],
        out_specs=pl.BlockSpec(memory_space=pl.ANY),
        scratch_shapes=[
            pltpu.VMEM((chunks, chunk, width), jnp.bfloat16),
            pltpu.SemaphoreType.DMA((chunks,)),
        ],
        name="pack",
    )(wanted, points[0])
    incoming = lax.all_to_all(outgoing.reshape(cells, slots, width), "row", 0, 0, tiled=True)
    incoming = incoming.reshape(rows, width)

    price_column = prices[0].reshape(centres, 1)
    packed, means, price, names = on_chip(
        functools.partial(start_kernel, cells),
        "start",
        (
            packed_shape,
            jax.ShapeDtypeStruct((share, width), jnp.float32),
            jax.ShapeDtypeStruct((share, 1), jnp.float32),
            jax.ShapeDtypeStruct((2, tops * count), jnp.float32),
        ),
        (False, False, False),
    )(wanted, centroids[0], price_column)

    groups = rows // LANES
    for sweep_index in range(STEPS):
        last = sweep_index == STEPS - 1
        first = sweep_index == 0
        sent = groups + 2 if first else groups
        logs = on_chip(
            functools.partial(stats_kernel, chunks, cells, share),
            "stats",
            jax.ShapeDtypeStruct((cells * sent, LANES), jnp.float32),
            (False, True, False) if first else None,
        )(packed, incoming, *((names,) if first else ()))
        logs = logs.reshape(cells, sent // 2, 2, LANES)
        logs = lax.all_to_all(logs, "row", 0, 0, tiled=True).reshape(cells * sent, LANES)
        if first:
            lines = rows // per_block
            hot, mask, empty = on_chip(
                functools.partial(index_kernel, capacity, per_block, tops),
                "index",
                (
                    jax.ShapeDtypeStruct((lines * tops, LANES), jnp.bfloat16),
                    jax.ShapeDtypeStruct((lines * tops, LANES), jnp.bfloat16),
                    jax.ShapeDtypeStruct((lines, LANES), jnp.float32),
                ),
            )(logs)
        sums = on_chip(
            functools.partial(sums_kernel, chunks, tops, per_block, cells, share),
            "sums",
            packed_shape,
            (False,) + (True,) * 5 if first else None,
        )(packed, incoming, logs, hot, mask, empty)
        pieces = lax.all_to_all(sums.reshape(copies, size, LANES), "col", 0, 0, tiled=True)
        piece, means, price = on_chip(
            functools.partial(update_kernel, target, last),
            "update",
            (
                packed_shape,
                jax.ShapeDtypeStruct((share, width), jnp.float32),
                jax.ShapeDtypeStruct((share, 1), jnp.float32),
            ),
            (True, False, False),
        )(pieces.reshape(copies * size, LANES), means, price)
        packed = lax.all_to_all(piece.reshape(copies, size, LANES), "col", 0, 0, tiled=True)
        packed = packed.reshape(copies * size, LANES)

    new_centroids, new_prices = on_chip(
        functools.partial(finish_kernel, share),
        "finish",
        (
            jax.ShapeDtypeStruct((centres, width), jnp.float32),
            jax.ShapeDtypeStruct((1, centres), jnp.float32),
        ),
    )(packed)
    return (new_centroids[None], new_prices)


def solution(mesh):
    placed = (P("col", "row", None), P("col", "row", None), P("row", None, None), P("row", None))
    return jax.shard_map(
        shards,
        mesh=mesh,
        in_specs=placed,
        out_specs=(P("row", None, None), P("row", None)),
        check_vma=False,
    )
```
